32 devices in a mesh: sx: 4 (over x, core), sy: 4 (over z), dp: 2 (over y).
Axes of the slice: x: 2, y: 2, z: 4, core: 2. Of those that a mesh axis runs over, the one named last changes fastest.
Arguments:
- tokens: bfloat16 [2, 8192, 1280], P('dp', ('sx', 'sy')), may hold values from -6 to 6
- lengths: int32 [2, 64], P('dp'), may hold values from 1 to 512, 8192 in all within a row
- ln_gain: float32 [1280], replicated, may hold values from 0.1 to 1.9
- w_qkv: bfloat16 [1280, 3840], P('dp'), may hold values from -4 to 4, as said below
- w_out: bfloat16 [1280, 1280], P('dp'), may hold values from -0.15625 to 0.15625
Outputs:
- hidden: bfloat16 [2, 8192, 1280], P('dp', ('sx', 'sy'))
- pooled: float32 [2, 64, 1280], P('dp')
The draws below stay inside these ranges and needn't reach their ends.
Inputs may be any that keep to these rules, and one draw needn't show every extreme that they name: The 64 lengths of a row sum to 8192; images are packed end to end in order. `w_qkv`: columns are queries, then keys, then values, each of 16 heads of 80 columns.
All inputs are finite; a program needn't handle non-finite values.
Results may differ from the reference program's by a relative error of at most 0.0051.
Values may be sent and summed in bfloat16 or wider, within the bound.
A program may use at most 128 MiB of HBM per device.

```python
import math
import jax
import jax.numpy as jnp
import numpy as np
from jax import lax

D = 1280
HEADS = 16
MAXLEN = 512
ROWS = 2
SEQ = 8192
IMAGES = 64


def draw_w_qkv(key, part):
    first = jax.random.fold_in(jax.random.fold_in(key, 11), 0)
    base = jax.random.normal(first, (D, 3 * D), jnp.float32) * D ** (-0.5)
    return jnp.clip(base, -4.0, 4.0).astype(jnp.bfloat16)


def block_levels(rng, dims, pieces, least, largest):
    def one(position, shards_of):
        steps = jax.random.uniform(jax.random.fold_in(jax.random.fold_in(rng, 6), position), (shards_of,), jnp.float32, least / len(pieces), largest / len(pieces))
        return jnp.repeat(jnp.exp(steps), dims[position] // shards_of).reshape((-1,) + (1,) * (len(dims) - position - 1))

    loudness = one(*pieces[0])
    for cut in pieces[1:]:
        loudness = loudness * one(*cut)
    return loudness


def split_up(number_of, total, limit, lean):
    portions = [(1 << 20) // math.isqrt(standing ** lean) + 1 for standing in range(2, number_of + 1)]
    spare, given = total - limit - (number_of - 1), [1] * (number_of - 1)
    while spare > 0:
        candidates = [i for i in range(number_of - 1) if given[i] < limit]
        whole, remaining = sum([portions[i] for i in candidates]), spare
        for i in candidates:
            extra = min(limit - given[i], max(1, remaining * portions[i] // whole), spare)
            given[i] = given[i] + extra
            spare = spare - extra
    return np.array([limit] + given)


def ragged_sizes(stream_key, number_of, total, limit, lean):
    if number_of == 2:
        one = jax.random.randint(stream_key, (), max(1, total - limit), min(limit, total - 1) + 1)
        return jnp.stack([one, total - one])
    sizes = jnp.asarray(split_up(number_of, total, limit, lean), jnp.int32)
    twos = (number_of - 1) // 2
    donor, taker = sizes[1:1 + 2 * twos:2], sizes[2:2 + 2 * twos:2]
    room = jnp.minimum(donor - 1, limit - taker)
    passed = jax.random.randint(jax.random.fold_in(stream_key, 1), (twos,), 0, 1 << 20) % (room + 1)
    sizes = sizes.at[1:1 + 2 * twos:2].set(donor - passed).at[2:2 + 2 * twos:2].set(taker + passed)
    return sizes[jax.random.permutation(jax.random.fold_in(stream_key, 2), number_of)]


def gaussian(stream_key, shape, scale, bound, cuts=(), held_as=jnp.bfloat16):
    result = scale * jax.random.normal(stream_key, shape, jnp.float32)
    if cuts:
        result = result * block_levels(stream_key, shape, cuts, -0.22, 0.18)
    return jnp.clip(result, -bound, bound).astype(held_as)


def setup_inputs(seed: int = 0) -> dict:
    splits = jax.random.split(jax.random.key(seed), 6)
    tokens = gaussian(splits[0], (ROWS, SEQ, D), 1.0, 6.0, ((0, 2), (1, 16)))
    lengths = jax.vmap(lambda own: ragged_sizes(own, IMAGES, SEQ, MAXLEN, 2))(jax.random.split(splits[1], ROWS)).reshape((ROWS, IMAGES)).astype(jnp.int32)
    ln_gain = jnp.clip(1.0 + 0.18 * jax.random.normal(splits[2], (D,), jnp.float32), 0.1, 1.9)
    w_qkv = draw_w_qkv(jax.random.fold_in(splits[5], 71), 0)
    w_out = gaussian(splits[4], (D, D), D ** -0.5, 0.15625, ((0, 2),))
    return {"tokens": tokens, "lengths": lengths, "ln_gain": ln_gain, "w_qkv": w_qkv, "w_out": w_out}


def image_ids(lengths, positions, total):
    offsets = jnp.cumsum(lengths) - lengths
    counted = lax.optimization_barrier(jnp.sum((offsets[None, :] <= positions[:, None]).astype(jnp.int32), axis=1)) - 1
    inside = (positions >= 0) & (positions < total)
    return jnp.where(inside, counted, -1).astype(jnp.int32)

def normalize(rows, ln_gain):
    values = rows.astype(jnp.float32)
    center = values - lax.optimization_barrier(jnp.mean(values, axis=-1, keepdims=True))
    spread = lax.optimization_barrier(jnp.mean(center * center, axis=-1, keepdims=True))
    return (center * lax.rsqrt(spread + 1e-05) * ln_gain).astype(jnp.bfloat16)

def attend(queries, keys, values, q_ids, k_ids, margin):
    length = queries.shape[0]
    heads = queries.shape[1]
    block = min(512, length)
    window = block + 2 * margin
    scale = queries.shape[2] ** (-0.5)

    def one_block(index):
        start = (index * block).astype(jnp.int32)
        q_blk = lax.dynamic_slice_in_dim(queries, start, block, 0)
        k_blk = lax.dynamic_slice_in_dim(keys, start, window, 0)
        v_blk = lax.dynamic_slice_in_dim(values, start, window, 0)
        q_lab = lax.dynamic_slice_in_dim(q_ids, start, block, 0)
        k_lab = lax.dynamic_slice_in_dim(k_ids, start, window, 0)
        allowed = q_lab[:, None] == k_lab[None, :]

        def one_head(head):
            q_head = lax.dynamic_index_in_dim(q_blk, head, 1, keepdims=False)
            k_head = lax.dynamic_index_in_dim(k_blk, head, 1, keepdims=False)
            v_head = lax.dynamic_index_in_dim(v_blk, head, 1, keepdims=False)
            scores = jnp.dot(q_head, k_head.T, preferred_element_type=jnp.float32) * scale
            scores = jnp.where(allowed, scores, -1e+30)
            top = lax.optimization_barrier(jnp.max(scores, axis=1, keepdims=True))
            weights = jnp.exp(scores - top)
            probs = (weights / lax.optimization_barrier(jnp.sum(weights, axis=1, keepdims=True))).astype(jnp.bfloat16)
            return jnp.dot(probs, v_head, preferred_element_type=jnp.float32).astype(jnp.bfloat16)
        outcome = lax.map(one_head, jnp.arange(heads, dtype=jnp.int32))
        return jnp.transpose(outcome, (1, 0, 2))
    blocks = lax.map(one_block, jnp.arange(length // block, dtype=jnp.int32))
    return blocks.reshape(length, heads, -1)

def reference(tokens, lengths, ln_gain, w_qkv, w_out):
    total = tokens.shape[1]
    width = tokens.shape[2]
    size = width // HEADS
    positions = jnp.arange(total, dtype=jnp.int32)
    extended = jnp.arange(total + 2 * MAXLEN, dtype=jnp.int32) - MAXLEN

    def one_row(pair):
        row, lens = pair
        normed = normalize(row, ln_gain)
        qkv = jnp.dot(normed, w_qkv, preferred_element_type=jnp.float32).astype(jnp.bfloat16)
        qkv = qkv.reshape(total, 3, HEADS, size)
        own_ids = image_ids(lens, positions, total)
        far_ids = image_ids(lens, extended, total)
        padding = jnp.zeros((MAXLEN, 3, HEADS, size), jnp.bfloat16)
        padded = jnp.concatenate([padding, qkv, padding], axis=0)
        context = attend(qkv[:, 0], padded[:, 1], padded[:, 2], own_ids, far_ids, MAXLEN)
        mixed = jnp.dot(context.reshape(total, width), w_out, preferred_element_type=jnp.float32)
        hidden = (row.astype(jnp.float32) + mixed).astype(jnp.bfloat16)
        onehot = (jnp.arange(IMAGES, dtype=jnp.int32)[:, None] == own_ids[None, :]).astype(jnp.bfloat16)
        sums = jnp.dot(onehot, hidden, preferred_element_type=jnp.float32)
        pooled = sums / lens.astype(jnp.float32)[:, None]
        return (hidden, pooled)
    hidden, pooled = lax.map(one_row, (tokens, lengths))
    return (hidden, pooled)
```

```python
import functools

import jax
import jax.numpy as jnp
from jax import lax
from jax.experimental import pallas as pl
from jax.experimental.pallas import tpu as pltpu
from jax.sharding import PartitionSpec as P

HEADS = 16
MAXLEN = 512
MESH = pl.DeviceIdType.MESH
GROUPS = 2
WIDE_CHUNKS = 3 * GROUPS
CHUNKS = 4 * GROUPS
HOP = 128
HOPS = MAXLEN // HOP
NEAR = 2
QBLOCK = 256
LANES = 128
ONES = 16
FAR = -1e30


def remote(src, dst, send, recv, device):
    return pltpu.make_async_remote_copy(
        src_ref=src, dst_ref=dst, send_sem=send, recv_sem=recv, device_id=device, device_id_type=MESH
    )


def head_window(head, size):
    low = head * size // LANES * LANES
    high = -(-(head + 1) * size // LANES) * LANES
    return low, high - low


def block_kernel(
    nx, ny, tok, lengths, gain, wq, wo, hidden, pooled,
    toks, normed, wq_full, wo_full, gains, keys, wide, turned, bias, top, acc, flat, context, hid, onehot, parts,
    landed, reduced, gathered,
    y_send, y_recv, x_send, x_recv, d_send, d_recv, h_send, h_recv, s_send, s_recv, g_send, g_recv, local_sem, out_sem,
):
    sx, sy, dp = lax.axis_index("sx"), lax.axis_index("sy"), lax.axis_index("dp")
    chips = nx // 2
    chip, core = sx // 2, lax.rem(sx, 2)
    count = nx * ny
    shard = sx * ny + sy
    first, last = shard == 0, shard == count - 1
    f32, bf16 = jnp.float32, jnp.bfloat16

    local, width = tok.shape
    long = toks.shape[0]
    size = width // HEADS
    half = wq.shape[0]
    quarter = half // nx
    cols = width // GROUPS
    team = HEADS // GROUPS
    images = pooled.shape[0]
    each = images // count
    blocks = local // QBLOCK
    factor = size ** (-0.5) * 1.4426950408889634

    def peer(step):
        other = lax.rem(shard + step, count)
        return other, (other // ny, lax.rem(other, ny), dp)

    prev_id, next_id = peer(count - 1)[1], peer(1)[1]
    y_id = (sx, sy, 1 - dp)
    partner = (chip * 2 + 1 - core, sy, dp)

    def chip_id(step):
        return (lax.rem(chip + step, chips) * 2 + core, sy, dp)

    barrier = pltpu.get_barrier_semaphore()
    for device in [y_id] + [peer(step)[1] for step in range(1, count)]:
        pl.semaphore_signal(barrier, inc=1, device_id=device, device_id_type=MESH)
    own_tokens = pltpu.make_async_copy(tok, toks.at[pl.ds(MAXLEN, local)], local_sem.at[0])
    mine = pl.ds(pl.multiple_of(dp * half, half), half)
    own_q = pltpu.make_async_copy(wq, wq_full.at[mine], local_sem.at[1])
    own_o = pltpu.make_async_copy(wo, wo_full.at[mine], local_sem.at[2])
    own_tokens.start()
    own_q.start()
    own_o.start()
    pl.semaphore_wait(barrier, count)

    def chunk(j):
        if j < WIDE_CHUNKS:
            return wq, wq_full, pl.ds(j % 3 * width + j // 3 * cols, cols)
        return wo, wo_full, pl.ds((j - WIDE_CHUNKS) * cols, cols)

    def rows(owner, slot):
        return pl.ds(pl.multiple_of(owner * half + slot * quarter, quarter), quarter)

    sends = []
    for j in range(CHUNKS):
        part, full, at = chunk(j)
        copy = remote(
            part.at[pl.ds(pl.multiple_of(sx * quarter, quarter), quarter), at],
            full.at[rows(dp, sx), at], y_send.at[j], y_recv.at[j], y_id,
        )
        copy.start()
        sends.append(copy)

    def place(side, hop):
        return MAXLEN + local + hop * HOP if side else MAXLEN - (hop + 1) * HOP

    def up(hop):
        return remote(
            tok.at[pl.ds(local - (hop + 1) * HOP, HOP)], toks.at[pl.ds(place(0, hop), HOP)],
            h_send.at[0, hop], h_recv.at[0, hop], next_id,
        )

    def down(hop):
        return remote(
            tok.at[pl.ds(hop * HOP, HOP)], toks.at[pl.ds(place(1, hop), HOP)],
            h_send.at[1, hop], h_recv.at[1, hop], prev_id,
        )

    @pl.when(jnp.logical_not(last))
    def _():
        for hop in range(HOPS):
            up(hop).start()

    @pl.when(jnp.logical_not(first))
    def _():
        for hop in range(HOPS):
            down(hop).start()

    @pl.when(first)
    def _():
        toks[pl.ds(0, MAXLEN)] = jnp.zeros((MAXLEN, width), toks.dtype)

    @pl.when(last)
    def _():
        toks[pl.ds(MAXLEN + local, MAXLEN)] = jnp.zeros((MAXLEN, width), toks.dtype)

    for i in range(width // LANES):
        gains[:, pl.ds(i * LANES, LANES)] = gain[pl.ds(i, 1), :]

    def norm(start, amount):
        step = 32

        @pl.loop(0, amount // step)
        def _(i):
            where = pl.ds(pl.multiple_of(start + i * step, step), step)
            values = toks[where].astype(f32)
            center = values - jnp.mean(values, axis=-1, keepdims=True)
            spread = jnp.mean(center * center, axis=-1, keepdims=True)
            normed[where] = (center * lax.rsqrt(spread + 1e-05) * gains[...]).astype(bf16)

    def project(start, amount, group, which):
        at = pl.ds(pl.multiple_of(which * width + group * cols, LANES), cols)
        return jnp.dot(normed[pl.ds(start, amount)], wq_full[:, at], preferred_element_type=f32)

    def project_q(start, amount, group):
        columns = (project(start, amount, group, 0) * factor).astype(bf16).T
        at = pl.ds(pl.multiple_of(start - MAXLEN, amount), amount)
        for head in range(team):
            low = head * size - head_window(head, size)[0]
            wide[group * team + head, pl.ds(low, size), at] = columns[head * size : (head + 1) * size]

    def project_k(start, amount, group):
        at = pl.ds(pl.multiple_of(group * cols, LANES), cols)
        keys[pl.ds(start, amount), at] = project(start, amount, group, 1).astype(bf16)

    def project_v(start, amount, group):
        columns = project(start, amount, group, 2).astype(bf16).T
        at = pl.ds(start, amount)
        for head in range(team):
            turned[group * team + head, pl.ds(0, size), at] = columns[head * size : (head + 1) * size]

    def attend(block, group, start, amount, fresh):
        queries = pl.ds(pl.multiple_of(block * QBLOCK, QBLOCK), QBLOCK)
        there = pl.ds(start, amount)
        shade = pl.ds(pl.multiple_of(start - block * QBLOCK, LANES), amount)
        for head in range(team):
            low, span = head_window(head, size)
            slot = group * team + head
            where = block * HEADS + slot
            scores = jnp.dot(
                keys[there, pl.ds(pl.multiple_of(group * cols + low, LANES), span)],
                wide[slot, pl.ds(0, span), queries], preferred_element_type=f32,
            ) + bias[block, shade]
            new = jnp.max(scores, axis=0, keepdims=True)
            if not fresh:
                old = top[where]
                new = jnp.maximum(old, new)
            probs = jnp.exp2(scores - new).astype(bf16)
            mixed = jnp.dot(turned[slot, :, there], probs, preferred_element_type=f32)
            if not fresh:
                mixed = acc[where] * jnp.exp2(old - new) + mixed
            acc[where] = mixed
            top[where] = new

    own_tokens.wait()
    norm(MAXLEN, local)

    wide[...] = jnp.zeros(wide.shape, bf16)
    turned[:, pl.ds(size, ONES), :] = jnp.ones((HEADS, ONES, long), bf16)
    row_lengths = lengths[...].astype(f32)
    to = lax.broadcasted_iota(jnp.int32, (images, images), 0)
    of = lax.broadcasted_iota(jnp.int32, (images, images), 1)
    offsets = jnp.sum(jnp.where(of < to, row_lengths, 0.0), axis=1, keepdims=True)
    amounts = jnp.sum(jnp.where(of == to, row_lengths, 0.0), axis=1, keepdims=True)
    ends = offsets + amounts
    base = shard * local
    spots = (base + lax.broadcasted_iota(jnp.int32, (1, local), 1)).astype(f32)
    inside = (offsets <= spots) & (spots < ends)
    onehot[...] = jnp.where(inside, 1.0, 0.0).astype(bf16)
    begin = jnp.max(jnp.where(inside, offsets, 0.0), axis=0, keepdims=True)
    end = jnp.max(jnp.where(inside, ends, 0.0), axis=0, keepdims=True)
    for block in range(blocks):
        mine_begin = begin[:, block * QBLOCK : (block + 1) * QBLOCK]
        mine_end = end[:, block * QBLOCK : (block + 1) * QBLOCK]
        step = 64

        @pl.loop(0, bias.shape[1] // step)
        def _(i):
            at = pl.multiple_of(i * step, step)
            spot = base - MAXLEN + block * QBLOCK + at + lax.broadcasted_iota(jnp.int32, (step, QBLOCK), 0)
            spot = spot.astype(f32)
            allowed = (spot >= mine_begin) & (spot < mine_end)
            bias[block, pl.ds(at, step)] = jnp.where(allowed, 0.0, FAR)

    def relay_y(j):
        here = chunk(j)[1].at[rows(1 - dp, sx), chunk(j)[2]]
        remote(here, here, y_send.at[j], y_recv.at[j], y_id).wait_recv()
        for step in range(1, chips):
            copy = remote(here, here, x_send.at[step - 1, j], x_recv.at[step - 1, j], chip_id(step))
            copy.start()
            sends.append(copy)
        copy = remote(here, here, d_send.at[0, j], d_recv.at[0, j], partner)
        copy.start()
        sends.append(copy)

    def relay_x(j):
        for step in range(1, chips):
            slot = lax.rem(chip + chips - step, chips) * 2 + core
            here = chunk(j)[1].at[rows(1 - dp, slot), chunk(j)[2]]
            remote(here, here, x_send.at[step - 1, j], x_recv.at[step - 1, j], y_id).wait_recv()
            copy = remote(here, here, d_send.at[step, j], d_recv.at[step, j], partner)
            copy.start()
            sends.append(copy)

    def complete(j):
        for step in range(chips):
            slot = lax.rem(chip + chips - step, chips) * 2 + 1 - core
            here = chunk(j)[1].at[rows(1 - dp, slot), chunk(j)[2]]
            remote(here, here, d_send.at[step, j], d_recv.at[step, j], partner).wait_recv()

    def own_chunk(j):
        group, which = j // 3, j % 3
        complete(j)

        @pl.loop(0, blocks)
        def _(i):
            start = pl.multiple_of(MAXLEN + i * QBLOCK, QBLOCK)
            (project_q, project_k, project_v)[which](start, QBLOCK, group)

        if which == 2:

            @pl.loop(0, blocks)
            def _(block):
                attend(block, group, MAXLEN, local, True)

    own_q.wait()
    for j in range(CHUNKS):
        relay_y(j)
        if j >= 1:
            relay_x(j - 1)
        if j >= 2:
            own_chunk(j - 2)

    def arrived(hop):
        for side in range(2):

            @pl.when(jnp.logical_not(last if side else first))
            def _():
                (down if side else up)(hop).wait_recv()

            norm(place(side, hop), HOP)

    for hop in range(NEAR):
        arrived(hop)
    near = NEAR * HOP

    @pl.loop(0, 2)
    def _(side):
        start = pl.multiple_of(MAXLEN - near + side * (local + near), near)

        @pl.loop(0, GROUPS)
        def _(group):
            project_k(start, near, group)
            project_v(start, near, group)

            @pl.loop(0, blocks)
            def _(block):
                attend(block, group, start, near, False)

    relay_x(CHUNKS - 1)
    for hop in range(NEAR, HOPS):
        arrived(hop)

        @pl.loop(0, 2)
        def _(side):
            start = pl.multiple_of(place(0, hop) + side * (place(1, hop) - place(0, hop)), HOP)

            @pl.loop(0, GROUPS)
            def _(group):
                project_k(start, HOP, group)
                project_v(start, HOP, group)
                attend(side * (blocks - 1), group, start, HOP, False)

    @pl.loop(0, blocks)
    def _(block):
        @pl.loop(0, GROUPS)
        def _(group):
            for head in range(team):
                where = block * HEADS + group * team + head
                share = 1.0 / acc[where, pl.ds(size, 1)]
                at = pl.ds(pl.multiple_of(group * cols + head * size, size), size)
                flat[at] = (acc[where, pl.ds(0, size)] * share).astype(bf16)

        context[pl.ds(pl.multiple_of(block * QBLOCK, QBLOCK), QBLOCK)] = flat[...].T

    own_o.wait()
    for j in range(WIDE_CHUNKS, CHUNKS):
        complete(j)
    tile = 256

    def put(c):
        at = pl.ds(pl.multiple_of(c * tile, tile), tile)
        return pltpu.make_async_copy(hid.at[:, at], hidden.at[:, at], out_sem.at[c])

    @pl.loop(0, width // tile)
    def _(c):
        at = pl.ds(pl.multiple_of(c * tile, tile), tile)
        mixed = jnp.dot(context[...], wo_full[:, at], preferred_element_type=f32)
        rounded = (toks[pl.ds(MAXLEN, local), at].astype(f32) + mixed).astype(bf16)
        hid[:, at] = rounded
        put(c).start()
        means = jnp.dot(onehot[...], rounded, preferred_element_type=f32) / amounts
        for p in range(count):
            parts[p, :, at] = means[p * each : (p + 1) * each].astype(bf16)

    copies = []
    for step in range(1, count):
        other, ident = peer(step)
        copy = remote(parts.at[other], landed.at[step - 1], s_send.at[step - 1], s_recv.at[step - 1], ident)
        copy.start()
        copies.append(copy)
    value = parts[shard].astype(f32)
    for step in range(1, count):
        copies[step - 1].wait_recv()
        value = value + landed[step - 1].astype(f32)
    reduced[...] = value.astype(bf16)
    gathered[shard] = value.astype(bf16)
    for step in range(1, count):
        copy = remote(reduced, gathered.at[shard], g_send.at[step - 1], g_recv.at[step - 1], peer(step)[1])
        copy.start()
        copies.append(copy)
    for step in range(1, count):
        source = peer(count - step)[0]
        remote(
            reduced, gathered.at[source], g_send.at[step - 1], g_recv.at[step - 1], peer(step)[1]
        ).wait_recv()
    for p in range(count):
        pooled[p * each : (p + 1) * each] = gathered[p].astype(f32)

    @pl.loop(0, width // tile)
    def _(c):
        put(c).wait()

    @pl.when(jnp.logical_not(last))
    def _():
        for hop in range(HOPS):
            up(hop).wait_send()

    @pl.when(jnp.logical_not(first))
    def _():
        for hop in range(HOPS):
            down(hop).wait_send()

    for copy in sends + copies:
        copy.wait_send()


def shards(nx, ny, tokens, lengths, ln_gain, w_qkv, w_out):
    local, width = tokens.shape[1:]
    images = lengths.shape[1]
    count = nx * ny
    chips = nx // 2
    each = images // count
    size = width // HEADS
    long = local + 2 * MAXLEN
    blocks = local // QBLOCK
    f32, bf16 = jnp.float32, jnp.bfloat16
    anywhere = pl.BlockSpec(memory_space=pl.ANY)
    vmem = pl.BlockSpec(memory_space=pltpu.VMEM)
    dma = pltpu.SemaphoreType.DMA
    hidden, pooled = pl.pallas_call(
        functools.partial(block_kernel, nx, ny),
        out_shape=(
            jax.ShapeDtypeStruct((local, width), bf16), jax.ShapeDtypeStruct((images, width), f32),
        ),
        in_specs=[anywhere, vmem, vmem, anywhere, anywhere],
        out_specs=(anywhere, vmem),
        scratch_shapes=[
            pltpu.VMEM((long, width), bf16), pltpu.VMEM((long, width), bf16),
            pltpu.VMEM((width, 3 * width), bf16), pltpu.VMEM((width, width), bf16),
            pltpu.VMEM((1, width), f32),
            pltpu.VMEM((long, width), bf16),
            pltpu.VMEM((HEADS, 2 * LANES, local), bf16),
            pltpu.VMEM((HEADS, size + ONES, long), bf16),
            pltpu.VMEM((blocks, QBLOCK + 2 * MAXLEN, QBLOCK), f32),
            pltpu.VMEM((blocks * HEADS, 1, QBLOCK), f32),
            pltpu.VMEM((blocks * HEADS, size + ONES, QBLOCK), f32),
            pltpu.VMEM((width, QBLOCK), bf16),
            pltpu.VMEM((local, width), bf16), pltpu.VMEM((local, width), bf16),
            pltpu.VMEM((images, local), bf16),
            pltpu.VMEM((count, each, width), bf16), pltpu.VMEM((count - 1, each, width), bf16),
            pltpu.VMEM((each, width), bf16), pltpu.VMEM((count, each, width), bf16),
            dma((CHUNKS,)), dma((CHUNKS,)),
            dma((max(chips - 1, 1), CHUNKS)), dma((max(chips - 1, 1), CHUNKS)),
            dma((chips, CHUNKS)), dma((chips, CHUNKS)),
            dma((2, HOPS)), dma((2, HOPS)),
            dma((count - 1,)), dma((count - 1,)), dma((count - 1,)), dma((count - 1,)),
            dma((3,)), dma((width // 256,)),
        ],
        compiler_params=pltpu.CompilerParams(
            collective_id=0, has_side_effects=True, vmem_limit_bytes=60 * 2**20
        ),
        name="block",
    )(tokens[0], lengths, ln_gain.reshape(width // LANES, LANES), w_qkv, w_out)
    return (hidden[None], pooled[None])


def solution(mesh):
    in_specs = (P("dp", ("sx", "sy"), None), P("dp", None), P(), P("dp", None), P("dp", None))
    out_specs = (P("dp", ("sx", "sy"), None), P("dp", None, None))
    body = functools.partial(shards, mesh.shape["sx"], mesh.shape["sy"])
    return jax.shard_map(body, mesh=mesh, in_specs=in_specs, out_specs=out_specs, check_vma=False)
```

```python
import functools

import jax
import jax.numpy as jnp
from jax import lax
from jax.experimental import pallas as pl
from jax.experimental.pallas import tpu as pltpu
from jax.sharding import PartitionSpec as P

HEADS = 16
MAXLEN = 512
MESH = pl.DeviceIdType.MESH
GROUPS = 2
WIDE_CHUNKS = 3 * GROUPS
CHUNKS = 4 * GROUPS
HOP = 128
HOPS = MAXLEN // HOP
NEAR = 2
QBLOCK = 256
LANES = 128
ONES = 16
FAR = -1e30


def remote(src, dst, send, recv, device):
    return pltpu.make_async_remote_copy(
        src_ref=src, dst_ref=dst, send_sem=send, recv_sem=recv, device_id=device, device_id_type=MESH
    )


def head_window(head, size):
    low = head * size // LANES * LANES
    high = -(-(head + 1) * size // LANES) * LANES
    return low, high - low


def block_kernel(
    nx, ny, tok, lengths_in, gain_in, wq, wo, hidden, pooled,
    lengths, gain, toks, normed, wq_full, wo_full, gains, keys, wide, turned, bias, top, acc, scores, probs, flat, context, onehot, sums, parts,
    landed, reduced, gathered,
    y_send, y_recv, x_send, x_recv, d_send, d_recv, h_send, h_recv, s_send, s_recv, g_send, g_recv, local_sem,
):
    sx, sy, dp = lax.axis_index("sx"), lax.axis_index("sy"), lax.axis_index("dp")
    chips = nx // 2
    chip, core = sx // 2, lax.rem(sx, 2)
    count = nx * ny
    shard = sx * ny + sy
    first, last = shard == 0, shard == count - 1
    f32, bf16 = jnp.float32, jnp.bfloat16

    local, width = tok.shape
    long = toks.shape[0]
    size = width // HEADS
    half = wq.shape[0]
    quarter = half // nx
    cols = width // GROUPS
    team = HEADS // GROUPS
    images = pooled.shape[0]
    each = images // count
    blocks = local // QBLOCK
    factor = size ** (-0.5) * 1.4426950408889634

    def peer(step):
        other = lax.rem(shard + step, count)
        return other, (other // ny, lax.rem(other, ny), dp)

    prev_id, next_id = peer(count - 1)[1], peer(1)[1]
    y_id = (sx, sy, 1 - dp)
    partner = (chip * 2 + 1 - core, sy, dp)

    def chip_id(step):
        return (lax.rem(chip + step, chips) * 2 + core, sy, dp)

    barrier = pltpu.get_barrier_semaphore()
    for device in [y_id] + [peer(step)[1] for step in range(1, count)]:
        pl.semaphore_signal(barrier, inc=1, device_id=device, device_id_type=MESH)
    own_tokens = pltpu.make_async_copy(tok, toks.at[pl.ds(MAXLEN, local)], local_sem.at[0])
    mine = pl.ds(pl.multiple_of(dp * half, half), half)

    def chunk(j):
        if j < WIDE_CHUNKS:
            return wq, pl.ds((j + 1) % 3 * width + j // 3 * cols, cols), wq_full, pl.ds(j * cols, cols)
        at = pl.ds((j - WIDE_CHUNKS) * cols, cols)
        return wo, at, wo_full, at

    own_weights = []
    for j in range(CHUNKS):
        part, at, full, to = chunk(j)
        own_weights.append(pltpu.make_async_copy(part.at[:, at], full.at[mine, to], local_sem.at[1 + j]))
    small = (
        pltpu.make_async_copy(lengths_in, lengths, local_sem.at[1 + CHUNKS]),
        pltpu.make_async_copy(gain_in, gain, local_sem.at[2 + CHUNKS]),
    )
    for copy in small:
        copy.start()
    own_tokens.start()
    for copy in own_weights:
        copy.start()
    pl.semaphore_wait(barrier, count)

    def rows(owner, slot):
        return pl.ds(pl.multiple_of(owner * half + slot * quarter, quarter), quarter)

    sends = []
    for j in range(CHUNKS):
        part, at, full, to = chunk(j)
        copy = remote(
            part.at[pl.ds(pl.multiple_of(sx * quarter, quarter), quarter), at],
            full.at[rows(dp, sx), to], y_send.at[j], y_recv.at[j], y_id,
        )
        copy.start()
        sends.append(copy)

    def place(side, hop):
        return MAXLEN + local + hop * HOP if side else MAXLEN - (hop + 1) * HOP

    def up(hop):
        return remote(
            tok.at[pl.ds(local - (hop + 1) * HOP, HOP)], toks.at[pl.ds(place(0, hop), HOP)],
            h_send.at[0, hop], h_recv.at[0, hop], next_id,
        )

    def down(hop):
        return remote(
            tok.at[pl.ds(hop * HOP, HOP)], toks.at[pl.ds(place(1, hop), HOP)],
            h_send.at[1, hop], h_recv.at[1, hop], prev_id,
        )

    for hop in range(HOPS):
        for side in range(2):

            @pl.when(jnp.logical_not(first if side else last))
            def _():
                (down if side else up)(hop).start()

    @pl.when(first)
    def _():
        toks[pl.ds(0, MAXLEN)] = jnp.zeros((MAXLEN, width), toks.dtype)

    @pl.when(last)
    def _():
        toks[pl.ds(MAXLEN + local, MAXLEN)] = jnp.zeros((MAXLEN, width), toks.dtype)

    for copy in small:
        copy.wait()
    for i in range(width // LANES):
        gains[:, pl.ds(i * LANES, LANES)] = gain[pl.ds(i, 1), :]

    def norm(start, amount):
        step = HOP

        @pl.loop(0, amount // step)
        def _(i):
            where = pl.ds(pl.multiple_of(start + i * step, step), step)
            values = toks[where].astype(f32)
            center = values - jnp.mean(values, axis=-1, keepdims=True)
            spread = jnp.mean(center * center, axis=-1, keepdims=True)
            normed[where] = (center * lax.rsqrt(spread + 1e-05) * gains[...]).astype(bf16)

    def project(start, amount, group, which, parts_of):
        at = pl.ds(pl.multiple_of((group * 3 + which) * cols, LANES), parts_of * cols)
        return jnp.dot(normed[pl.ds(start, amount)], wq_full[:, at], preferred_element_type=f32)

    def project_q(start, amount, group):
        columns = (project(start, amount, group, 2, 1) * factor).astype(bf16).T
        at = pl.ds(pl.multiple_of(start - MAXLEN, amount), amount)
        for head in range(team):
            low = head * size - head_window(head, size)[0]
            wide[group * team + head, pl.ds(low, size), at] = columns[head * size : (head + 1) * size]

    def project_kv(start, amount, group):
        both = project(start, amount, group, 0, 2).astype(bf16)
        here = pl.ds(start, amount)
        keys[here, pl.ds(pl.multiple_of(group * cols, LANES), cols)] = both[:, :cols]
        columns = both[:, cols:].T
        for head in range(team):
            turned[group * team + head, pl.ds(0, size), here] = columns[head * size : (head + 1) * size]

    def attend(block, group, start, amount, fresh, lane=0, lanes=QBLOCK):
        queries = pl.ds(pl.multiple_of(block * QBLOCK + lane, LANES), lanes)
        within = pl.ds(lane, lanes)
        there = pl.ds(start, amount)
        shade = pl.ds(pl.multiple_of(start - block * QBLOCK, LANES), amount)
        some = (pl.ds(0, amount), pl.ds(0, lanes))
        tops, shrinks = [], []
        for head in range(team):
            low, span = head_window(head, size)
            slot = group * team + head
            found = jnp.dot(
                keys[there, pl.ds(pl.multiple_of(group * cols + low, LANES), span)],
                wide[slot, pl.ds(0, span), queries], preferred_element_type=f32,
            ) + bias[block, shade, within]
            scores[(head,) + some] = found
            tops.append(jnp.max(found, axis=0, keepdims=True))
        for head in range(team):
            where = block * HEADS + group * team + head
            new = tops[head]
            if not fresh:
                old = top[where, :, within]
                new = jnp.maximum(old, new)
                shrinks.append(jnp.exp2(old - new))
            top[where, :, within] = new
            probs[(head,) + some] = jnp.exp2(scores[(head,) + some] - new).astype(bf16)
        for head in range(team):
            slot = group * team + head
            where = block * HEADS + slot
            mixed = jnp.dot(turned[slot, :, there], probs[(head,) + some], preferred_element_type=f32)
            if not fresh:
                mixed = acc[where, :, within] * shrinks[head] + mixed
            acc[where, :, within] = mixed

    own_tokens.wait()
    norm(MAXLEN, local)

    wide[...] = jnp.zeros(wide.shape, bf16)
    turned[:, pl.ds(size, ONES), :] = jnp.ones((HEADS, ONES, long), bf16)
    row_lengths = lengths[...].astype(f32)
    to = lax.broadcasted_iota(jnp.int32, (images, images), 0)
    of = lax.broadcasted_iota(jnp.int32, (images, images), 1)
    offsets = jnp.sum(jnp.where(of < to, row_lengths, 0.0), axis=1, keepdims=True)
    amounts = jnp.sum(jnp.where(of == to, row_lengths, 0.0), axis=1, keepdims=True)
    ends = offsets + amounts
    base = shard * local
    spots = (base + lax.broadcasted_iota(jnp.int32, (1, local), 1)).astype(f32)
    inside = (offsets <= spots) & (spots < ends)
    onehot[...] = jnp.where(inside, 1.0, 0.0).astype(bf16)
    begin = jnp.max(jnp.where(inside, offsets, 0.0), axis=0, keepdims=True)
    end = jnp.max(jnp.where(inside, ends, 0.0), axis=0, keepdims=True)
    for block in range(blocks):
        mine_begin = begin[:, block * QBLOCK : (block + 1) * QBLOCK]
        mine_end = end[:, block * QBLOCK : (block + 1) * QBLOCK]
        step = 64

        @pl.loop(0, bias.shape[1] // step)
        def _(i):
            at = pl.multiple_of(i * step, step)
            spot = base - MAXLEN + block * QBLOCK + at + lax.broadcasted_iota(jnp.int32, (step, QBLOCK), 0)
            spot = spot.astype(f32)
            allowed = (spot >= mine_begin) & (spot < mine_end)
            bias[block, pl.ds(at, step)] = jnp.where(allowed, 0.0, FAR)

    def relay_y(j):
        here = chunk(j)[2].at[rows(1 - dp, sx), chunk(j)[3]]
        remote(here, here, y_send.at[j], y_recv.at[j], y_id).wait_recv()
        for step in range(1, chips):
            copy = remote(here, here, x_send.at[step - 1, j], x_recv.at[step - 1, j], chip_id(step))
            copy.start()
            sends.append(copy)
        copy = remote(here, here, d_send.at[0, j], d_recv.at[0, j], partner)
        copy.start()
        sends.append(copy)

    def relay_x(j):
        for step in range(1, chips):
            slot = lax.rem(chip + chips - step, chips) * 2 + core
            here = chunk(j)[2].at[rows(1 - dp, slot), chunk(j)[3]]
            remote(here, here, x_send.at[step - 1, j], x_recv.at[step - 1, j], y_id).wait_recv()
            copy = remote(here, here, d_send.at[step, j], d_recv.at[step, j], partner)
            copy.start()
            sends.append(copy)

    def complete(j):
        for step in range(chips):
            slot = lax.rem(chip + chips - step, chips) * 2 + 1 - core
            here = chunk(j)[2].at[rows(1 - dp, slot), chunk(j)[3]]
            remote(here, here, d_send.at[step, j], d_recv.at[step, j], partner).wait_recv()

    def arrived(hop):
        for side in range(2):

            @pl.when(jnp.logical_not(last if side else first))
            def _():
                (down if side else up)(hop).wait_recv()

            norm(place(side, hop), HOP)

    near = NEAR * HOP

    near_starts = (MAXLEN - near, MAXLEN + local)

    def near_kv(group):
        for side in range(2):
            project_kv(near_starts[side], near, group)

    def near_attend(group):
        @pl.loop(0, 2)
        def _(side):
            start = pl.multiple_of(near_starts[0] + side * (near_starts[1] - near_starts[0]), near)

            @pl.loop(0, blocks)
            def _(block):
                attend(block, group, start, near, False)

    def own_attend(group):
        @pl.loop(0, blocks)
        def _(block):
            attend(block, group, MAXLEN, local, True)

    def ready(*chunks):
        for j in chunks:
            complete(j)
            own_weights[j].wait()

    def far(hop):
        arrived(hop)

        @pl.loop(0, GROUPS)
        def _(group):
            for side in range(2):
                project_kv(place(side, hop), HOP, group)
            for side in range(2):
                lanes = min(QBLOCK, (HOPS - hop) * HOP)
                attend(side * (blocks - 1), group, place(side, hop), HOP, False, side * (QBLOCK - lanes), lanes)

    tile = 256

    def finish(start, amount):
        for at in range(start, start + amount, HOP):
            block, lane = at // QBLOCK, at % QBLOCK

            @pl.loop(0, GROUPS)
            def _(group):
                for head in range(team):
                    where = block * HEADS + group * team + head
                    share = 1.0 / acc[where, pl.ds(size, 1), pl.ds(lane, HOP)]
                    rows_at = pl.ds(pl.multiple_of(group * cols + head * size, size), size)
                    flat[rows_at] = (acc[where, pl.ds(0, size), pl.ds(lane, HOP)] * share).astype(bf16)

            context[pl.ds(at, HOP)] = flat[...].T

    def emit(start, amount):
        where = pl.ds(start, amount)

        @pl.loop(0, width // tile)
        def _(c):
            at = pl.ds(pl.multiple_of(c * tile, tile), tile)
            mixed = jnp.dot(context[where], wo_full[:, at], preferred_element_type=f32)
            hidden[where, at] = (toks[pl.ds(MAXLEN + start, amount), at].astype(f32) + mixed).astype(bf16)

    def relay(j):
        relay_y(j)
        if j:
            relay_x(j - 1)

    for j in range(4):
        relay(j)
    ready(0, 1)
    project_kv(MAXLEN, local, 0)
    ready(2)
    project_q(MAXLEN, local, 0)
    relay(4)
    own_attend(0)
    relay(5)
    arrived(0)
    relay_x(5)
    arrived(1)
    near_kv(0)
    ready(3, 4)
    project_kv(MAXLEN, local, 1)
    relay_y(6)
    near_attend(0)
    ready(5)
    project_q(MAXLEN, local, 1)
    relay_x(6)
    relay_y(7)
    own_attend(1)
    near_kv(1)
    relay_x(7)
    near_attend(1)
    for hop in range(NEAR, HOPS - 1):
        far(hop)
    ready(*range(WIDE_CHUNKS, CHUNKS))
    finish(HOP, local - 2 * HOP)
    emit(HOP, local - 2 * HOP)
    far(HOPS - 1)
    for start in (0, local - HOP):
        finish(start, HOP)
    for start in (0, local - HOP):
        emit(start, HOP)

    sums[...] = jnp.dot(onehot[...], hidden[...], preferred_element_type=f32) / amounts
    for p in range(count):
        parts[p] = sums[p * each : (p + 1) * each].astype(bf16)

    copies = []
    for step in range(1, count):
        other, ident = peer(step)
        copy = remote(parts.at[other], landed.at[step - 1], s_send.at[step - 1], s_recv.at[step - 1], ident)
        copy.start()
        copies.append(copy)
    value = parts[shard].astype(f32)
    for step in range(1, count):
        copies[step - 1].wait_recv()
        value = value + landed[step - 1].astype(f32)
    reduced[...] = value.astype(bf16)
    gathered[shard] = value.astype(bf16)
    for step in range(1, count):
        copy = remote(reduced, gathered.at[shard], g_send.at[step - 1], g_recv.at[step - 1], peer(step)[1])
        copy.start()
        copies.append(copy)
    for step in range(1, count):
        source = peer(count - step)[0]
        remote(
            reduced, gathered.at[source], g_send.at[step - 1], g_recv.at[step - 1], peer(step)[1]
        ).wait_recv()
    for p in range(count):
        pooled[p * each : (p + 1) * each] = gathered[p].astype(f32)


    for side in range(2):

        @pl.when(jnp.logical_not(first if side else last))
        def _():
            for hop in range(HOPS):
                (down if side else up)(hop).wait_send()

    for copy in sends + copies:
        copy.wait_send()


def shards(nx, ny, tokens, lengths, ln_gain, w_qkv, w_out):
    local, width = tokens.shape[1:]
    images = lengths.shape[1]
    count = nx * ny
    chips = nx // 2
    each = images // count
    size = width // HEADS
    long = local + 2 * MAXLEN
    blocks = local // QBLOCK
    team = HEADS // GROUPS
    f32, bf16 = jnp.float32, jnp.bfloat16
    hbm = pl.BlockSpec(memory_space=pltpu.HBM)
    vmem = pl.BlockSpec(memory_space=pltpu.VMEM)
    dma = pltpu.SemaphoreType.DMA
    hidden, pooled = pl.pallas_call(
        functools.partial(block_kernel, nx, ny),
        out_shape=(
            jax.ShapeDtypeStruct((local, width), bf16), jax.ShapeDtypeStruct((images, width), f32),
        ),
        in_specs=[hbm] * 5,
        out_specs=(vmem, vmem),
        scratch_shapes=[
            pltpu.VMEM((1, images), jnp.int32), pltpu.VMEM((width // LANES, LANES), f32),
            pltpu.VMEM((long, width), bf16), pltpu.VMEM((long, width), bf16),
            pltpu.VMEM((width, 3 * width), bf16), pltpu.VMEM((width, width), bf16),
            pltpu.VMEM((1, width), f32),
            pltpu.VMEM((long, width), bf16),
            pltpu.VMEM((HEADS, 2 * LANES, local), bf16),
            pltpu.VMEM((HEADS, size + ONES, long), bf16),
            pltpu.VMEM((blocks, QBLOCK + 2 * MAXLEN, QBLOCK), f32),
            pltpu.VMEM((blocks * HEADS, 1, QBLOCK), f32),
            pltpu.VMEM((blocks * HEADS, size + ONES, QBLOCK), f32),
            pltpu.VMEM((team, local, QBLOCK), f32), pltpu.VMEM((team, local, QBLOCK), bf16),
            pltpu.VMEM((width, HOP), bf16),
            pltpu.VMEM((local, width), bf16),
            pltpu.VMEM((images, local), bf16), pltpu.VMEM((images, width), f32),
            pltpu.VMEM((count, each, width), bf16), pltpu.VMEM((count - 1, each, width), bf16),
            pltpu.VMEM((each, width), bf16), pltpu.VMEM((count, each, width), bf16),
            dma((CHUNKS,)), dma((CHUNKS,)),
            dma((max(chips - 1, 1), CHUNKS)), dma((max(chips - 1, 1), CHUNKS)),
            dma((chips, CHUNKS)), dma((chips, CHUNKS)),
            dma((2, HOPS)), dma((2, HOPS)),
            dma((count - 1,)), dma((count - 1,)), dma((count - 1,)), dma((count - 1,)),
            dma((3 + CHUNKS,)),
        ],
        compiler_params=pltpu.CompilerParams(
            collective_id=0, has_side_effects=True, vmem_limit_bytes=51 * 2**20 + count * 2**16
        ),
        name="block",
    )(tokens[0], lengths, ln_gain.reshape(width // LANES, LANES), w_qkv, w_out)
    return (hidden[None], pooled[None])


def solution(mesh):
    in_specs = (P("dp", ("sx", "sy"), None), P("dp", None), P(), P("dp", None), P("dp", None))
    out_specs = (P("dp", ("sx", "sy"), None), P("dp", None, None))
    body = functools.partial(shards, mesh.shape["sx"], mesh.shape["sy"])
    return jax.shard_map(body, mesh=mesh, in_specs=in_specs, out_specs=out_specs, check_vma=False)
```

```python
import functools

import jax
import jax.numpy as jnp
from jax import lax
from jax.experimental import pallas as pl
from jax.experimental.pallas import tpu as pltpu
from jax.sharding import PartitionSpec as P

HEADS = 16
MAXLEN = 512
MESH = pl.DeviceIdType.MESH
GROUPS = 2
WIDE_CHUNKS = 3 * GROUPS
CHUNKS = 4 * GROUPS
HOP = 128
HOPS = MAXLEN // HOP
NEAR = 2
QBLOCK = 256
LANES = 128
ONES = 16
FAR = -1e30


def remote(src, dst, send, recv, device):
    return pltpu.make_async_remote_copy(
        src_ref=src, dst_ref=dst, send_sem=send, recv_sem=recv, device_id=device, device_id_type=MESH
    )


def head_window(head, size):
    low = head * size // LANES * LANES
    high = -(-(head + 1) * size // LANES) * LANES
    return low, high - low


def block_kernel(
    nx, ny, tok, lengths_in, gain_in, wq, wo, hidden, pooled,
    lengths, gain, toks, normed, wq_full, wo_full, gains, keys, wide, turned, bias, top, acc, scores, probs, flat, context, onehot, sums, parts,
    landed, reduced, gathered,
    y_send, y_recv, x_send, x_recv, d_send, d_recv, h_send, h_recv, s_send, s_recv, g_send, g_recv, local_sem,
):
    sx, sy, dp = lax.axis_index("sx"), lax.axis_index("sy"), lax.axis_index("dp")
    chips = nx // 2
    chip, core = sx // 2, lax.rem(sx, 2)
    count = nx * ny
    shard = sx * ny + sy
    first, last = shard == 0, shard == count - 1
    f32, bf16 = jnp.float32, jnp.bfloat16

    local, width = tok.shape
    long = toks.shape[0]
    size = width // HEADS
    half = wq.shape[0]
    quarter = half // nx
    cols = width // GROUPS
    team = HEADS // GROUPS
    images = pooled.shape[0]
    each = images // count
    blocks = local // QBLOCK
    factor = size ** (-0.5) * 1.4426950408889634

    def peer(step):
        other = lax.rem(shard + step, count)
        return other, (other // ny, lax.rem(other, ny), dp)

    prev_id, next_id = peer(count - 1)[1], peer(1)[1]
    y_id = (sx, sy, 1 - dp)
    partner = (chip * 2 + 1 - core, sy, dp)

    def chip_id(step):
        return (lax.rem(chip + step, chips) * 2 + core, sy, dp)

    barrier = pltpu.get_barrier_semaphore()
    for device in [y_id] + [peer(step)[1] for step in range(1, count)]:
        pl.semaphore_signal(barrier, inc=1, device_id=device, device_id_type=MESH)
    own_tokens = pltpu.make_async_copy(tok, toks.at[pl.ds(MAXLEN, local)], local_sem.at[0])
    mine = pl.ds(pl.multiple_of(dp * half, half), half)

    def chunk(j):
        if j < WIDE_CHUNKS:
            return wq, pl.ds((j + 1) % 3 * width + j // 3 * cols, cols), wq_full, pl.ds(j * cols, cols)
        at = pl.ds((j - WIDE_CHUNKS) * cols, cols)
        return wo, at, wo_full, at

    own_weights = []
    for j in range(CHUNKS):
        part, at, full, to = chunk(j)
        own_weights.append(pltpu.make_async_copy(part.at[:, at], full.at[mine, to], local_sem.at[1 + j]))
    small = (
        pltpu.make_async_copy(lengths_in, lengths, local_sem.at[1 + CHUNKS]),
        pltpu.make_async_copy(gain_in, gain, local_sem.at[2 + CHUNKS]),
    )
    for copy in small:
        copy.start()
    own_tokens.start()
    for copy in own_weights:
        copy.start()
    pl.semaphore_wait(barrier, count)

    def rows(owner, slot):
        return pl.ds(pl.multiple_of(owner * half + slot * quarter, quarter), quarter)

    sends = []
    for j in range(CHUNKS):
        part, at, full, to = chunk(j)
        copy = remote(
            part.at[pl.ds(pl.multiple_of(sx * quarter, quarter), quarter), at],
            full.at[rows(dp, sx), to], y_send.at[j], y_recv.at[j], y_id,
        )
        copy.start()
        sends.append(copy)

    def place(side, hop):
        return MAXLEN + local + hop * HOP if side else MAXLEN - (hop + 1) * HOP

    def up(hop):
        return remote(
            tok.at[pl.ds(local - (hop + 1) * HOP, HOP)], toks.at[pl.ds(place(0, hop), HOP)],
            h_send.at[0, hop], h_recv.at[0, hop], next_id,
        )

    def down(hop):
        return remote(
            tok.at[pl.ds(hop * HOP, HOP)], toks.at[pl.ds(place(1, hop), HOP)],
            h_send.at[1, hop], h_recv.at[1, hop], prev_id,
        )

    for hop in range(HOPS):
        for side in range(2):

            @pl.when(jnp.logical_not(first if side else last))
            def _():
                (down if side else up)(hop).start()

    @pl.when(first)
    def _():
        toks[pl.ds(0, MAXLEN)] = jnp.zeros((MAXLEN, width), toks.dtype)

    @pl.when(last)
    def _():
        toks[pl.ds(MAXLEN + local, MAXLEN)] = jnp.zeros((MAXLEN, width), toks.dtype)

    for copy in small:
        copy.wait()
    for i in range(width // LANES):
        gains[:, pl.ds(i * LANES, LANES)] = gain[pl.ds(i, 1), :]

    def norm(start, amount, to):
        step = HOP

        @pl.loop(0, amount // step)
        def _(i):
            where = pl.ds(pl.multiple_of(start + i * step, step), step)
            values = toks[where].astype(f32)
            center = values - jnp.mean(values, axis=-1, keepdims=True)
            spread = jnp.mean(center * center, axis=-1, keepdims=True)
            normed[pl.ds(pl.multiple_of(to + i * step, step), step)] = (center * lax.rsqrt(spread + 1e-05) * gains[...]).astype(bf16)

    def project(start, amount, group, which, parts_of):
        at = pl.ds(pl.multiple_of((group * 3 + which) * cols, LANES), parts_of * cols)
        return jnp.dot(normed[pl.ds(start, amount)], wq_full[:, at], preferred_element_type=f32)

    def project_q(start, amount, group):
        columns = (project(start, amount, group, 2, 1) * factor).astype(bf16).T
        at = pl.ds(pl.multiple_of(start - MAXLEN, amount), amount)
        for head in range(team):
            low = head * size - head_window(head, size)[0]
            wide[group * team + head, pl.ds(low, size), at] = columns[head * size : (head + 1) * size]

    def project_kv(start, amount, group, places=None):
        both = project(start, amount, group, 0, 2).astype(bf16)
        columns = both[:, cols:].T
        places = places or (start,)
        each_part = amount // len(places)
        for i, to in enumerate(places):
            part = slice(i * each_part, (i + 1) * each_part)
            here = pl.ds(to, each_part)
            keys[here, pl.ds(pl.multiple_of(group * cols, LANES), cols)] = both[part, :cols]
            for head in range(team):
                turned[group * team + head, pl.ds(0, size), here] = columns[head * size : (head + 1) * size, part]

    def attend(block, group, segments, fresh, lane=0, lanes=QBLOCK):
        queries = pl.ds(pl.multiple_of(block * QBLOCK + lane, LANES), lanes)
        within = pl.ds(lane, lanes)
        total = sum(amount for _, amount in segments)
        offsets_at = [sum(amount for _, amount in segments[:i]) for i in range(len(segments))]
        some = (pl.ds(0, total), pl.ds(0, lanes))
        tops, shrinks = [], []
        for head in range(team):
            low, span = head_window(head, size)
            slot = group * team + head
            most = None
            for at, (start, amount) in zip(offsets_at, segments):
                shade = pl.ds(pl.multiple_of(start - block * QBLOCK, LANES), amount)
                found = jnp.dot(
                    keys[pl.ds(start, amount), pl.ds(pl.multiple_of(group * cols + low, LANES), span)],
                    wide[slot, pl.ds(0, span), queries], preferred_element_type=f32,
                ) + bias[block, shade, within]
                scores[head, pl.ds(at, amount), pl.ds(0, lanes)] = found
                peak = jnp.max(found, axis=0, keepdims=True)
                most = peak if most is None else jnp.maximum(most, peak)
            tops.append(most)
        for head in range(team):
            where = block * HEADS + group * team + head
            new = tops[head]
            if not fresh:
                old = top[where, :, within]
                new = jnp.maximum(old, new)
                shrinks.append(jnp.exp2(old - new))
            top[where, :, within] = new
            probs[(head,) + some] = jnp.exp2(scores[(head,) + some] - new).astype(bf16)
        for head in range(team):
            slot = group * team + head
            where = block * HEADS + slot
            mixed = None
            for at, (start, amount) in zip(offsets_at, segments):
                part = jnp.dot(
                    turned[slot, :, pl.ds(start, amount)], probs[head, pl.ds(at, amount), pl.ds(0, lanes)],
                    preferred_element_type=f32,
                )
                mixed = part if mixed is None else mixed + part
            if not fresh:
                mixed = acc[where, :, within] * shrinks[head] + mixed
            acc[where, :, within] = mixed

    own_tokens.wait()
    norm(MAXLEN, local, MAXLEN)

    wide[...] = jnp.zeros(wide.shape, bf16)
    turned[:, pl.ds(size, ONES), :] = jnp.ones((HEADS, ONES, long), bf16)
    row_lengths = lengths[...].astype(f32)
    to = lax.broadcasted_iota(jnp.int32, (images, images), 0)
    of = lax.broadcasted_iota(jnp.int32, (images, images), 1)
    offsets = jnp.sum(jnp.where(of < to, row_lengths, 0.0), axis=1, keepdims=True)
    amounts = jnp.sum(jnp.where(of == to, row_lengths, 0.0), axis=1, keepdims=True)
    ends = offsets + amounts
    base = shard * local
    spots = (base + lax.broadcasted_iota(jnp.int32, (1, local), 1)).astype(f32)
    inside = (offsets <= spots) & (spots < ends)
    onehot[...] = jnp.where(inside, 1.0, 0.0).astype(bf16)
    begin = jnp.max(jnp.where(inside, offsets, 0.0), axis=0, keepdims=True)
    end = jnp.max(jnp.where(inside, ends, 0.0), axis=0, keepdims=True)
    for block in range(blocks):
        mine_begin = begin[:, block * QBLOCK : (block + 1) * QBLOCK]
        mine_end = end[:, block * QBLOCK : (block + 1) * QBLOCK]
        step = 64

        @pl.loop(0, bias.shape[1] // step)
        def _(i):
            at = pl.multiple_of(i * step, step)
            spot = base - MAXLEN + block * QBLOCK + at + lax.broadcasted_iota(jnp.int32, (step, QBLOCK), 0)
            spot = spot.astype(f32)
            allowed = (spot >= mine_begin) & (spot < mine_end)
            bias[block, pl.ds(at, step)] = jnp.where(allowed, 0.0, FAR)

    def relay_y(j):
        here = chunk(j)[2].at[rows(1 - dp, sx), chunk(j)[3]]
        remote(here, here, y_send.at[j], y_recv.at[j], y_id).wait_recv()
        for step in range(1, chips):
            copy = remote(here, here, x_send.at[step - 1, j], x_recv.at[step - 1, j], chip_id(step))
            copy.start()
            sends.append(copy)
        copy = remote(here, here, d_send.at[0, j], d_recv.at[0, j], partner)
        copy.start()
        sends.append(copy)

    def relay_x(j):
        for step in range(1, chips):
            slot = lax.rem(chip + chips - step, chips) * 2 + core
            here = chunk(j)[2].at[rows(1 - dp, slot), chunk(j)[3]]
            remote(here, here, x_send.at[step - 1, j], x_recv.at[step - 1, j], y_id).wait_recv()
            copy = remote(here, here, d_send.at[step, j], d_recv.at[step, j], partner)
            copy.start()
            sends.append(copy)

    def complete(j):
        for step in range(chips):
            slot = lax.rem(chip + chips - step, chips) * 2 + 1 - core
            here = chunk(j)[2].at[rows(1 - dp, slot), chunk(j)[3]]
            remote(here, here, d_send.at[step, j], d_recv.at[step, j], partner).wait_recv()

    def arrived(hop):
        for side in range(2):

            @pl.when(jnp.logical_not(last if side else first))
            def _():
                (down if side else up)(hop).wait_recv()

            norm(place(side, hop), HOP, place(side, hop) if hop < NEAR else side * HOP)

    near = NEAR * HOP

    near_starts = (MAXLEN - near, MAXLEN + local)

    def near_kv(group):
        for side in range(2):
            project_kv(near_starts[side], near, group)

    def near_attend(group):
        @pl.loop(0, blocks)
        def _(block):
            attend(block, group, [(start, near) for start in near_starts], False)

    def own_attend(group):
        @pl.loop(0, blocks)
        def _(block):
            attend(block, group, [(MAXLEN, local)], True)

    def ready(*chunks):
        for j in chunks:
            complete(j)
            own_weights[j].wait()

    def far(hop):
        arrived(hop)

        @pl.loop(0, GROUPS)
        def _(group):
            project_kv(0, 2 * HOP, group, (place(0, hop), place(1, hop)))
            for side in range(2):
                lanes = min(QBLOCK, (HOPS - hop) * HOP)
                spot = [(place(side, hop), HOP)]
                attend(side * (blocks - 1), group, spot, False, side * (QBLOCK - lanes), lanes)

    tile = cols

    def finish(start, amount):
        for at in range(start, start + amount, HOP):
            block, lane = at // QBLOCK, at % QBLOCK

            @pl.loop(0, GROUPS)
            def _(group):
                for head in range(team):
                    where = block * HEADS + group * team + head
                    share = 1.0 / acc[where, pl.ds(size, 1), pl.ds(lane, HOP)]
                    rows_at = pl.ds(pl.multiple_of(group * cols + head * size, size), size)
                    flat[rows_at] = (acc[where, pl.ds(0, size), pl.ds(lane, HOP)] * share).astype(bf16)

            context[pl.ds(at, HOP)] = flat[...].T

    def emit(starts, amount):
        @pl.loop(0, width // tile)
        def _(c):
            at = pl.ds(pl.multiple_of(c * tile, LANES), tile)
            lhs = jnp.concatenate([context[pl.ds(start, amount)] for start in starts], axis=0)
            mixed = jnp.dot(lhs, wo_full[:, at], preferred_element_type=f32)
            for i, start in enumerate(starts):
                residual = toks[pl.ds(MAXLEN + start, amount), at].astype(f32)
                hidden[pl.ds(start, amount), at] = (residual + mixed[i * amount : (i + 1) * amount]).astype(bf16)

    def relay(j):
        relay_y(j)
        if j:
            relay_x(j - 1)

    for j in range(4):
        relay(j)
    ready(0, 1)
    project_kv(MAXLEN, local, 0)
    ready(2)
    project_q(MAXLEN, local, 0)
    relay(4)
    own_attend(0)
    relay(5)
    arrived(0)
    relay_x(5)
    arrived(1)
    near_kv(0)
    ready(3, 4)
    project_kv(MAXLEN, local, 1)
    relay_y(6)
    near_attend(0)
    ready(5)
    project_q(MAXLEN, local, 1)
    relay_x(6)
    relay_y(7)
    own_attend(1)
    near_kv(1)
    relay_x(7)
    near_attend(1)
    for hop in range(NEAR, HOPS - 1):
        far(hop)
    ready(*range(WIDE_CHUNKS, CHUNKS))
    finish(HOP, local - 2 * HOP)
    emit((HOP,), local - 2 * HOP)
    far(HOPS - 1)
    for start in (0, local - HOP):
        finish(start, HOP)
    emit((0, local - HOP), HOP)

    sums[...] = jnp.dot(onehot[...], hidden[...], preferred_element_type=f32) / amounts
    for p in range(count):
        parts[p] = sums[p * each : (p + 1) * each].astype(bf16)

    copies = []
    for step in range(1, count):
        other, ident = peer(step)
        copy = remote(parts.at[other], landed.at[step - 1], s_send.at[step - 1], s_recv.at[step - 1], ident)
        copy.start()
        copies.append(copy)
    value = parts[shard].astype(f32)
    for step in range(1, count):
        copies[step - 1].wait_recv()
        value = value + landed[step - 1].astype(f32)
    reduced[...] = value.astype(bf16)
    gathered[shard] = value.astype(bf16)
    for step in range(1, count):
        copy = remote(reduced, gathered.at[shard], g_send.at[step - 1], g_recv.at[step - 1], peer(step)[1])
        copy.start()
        copies.append(copy)
    for step in range(1, count):
        source = peer(count - step)[0]
        remote(
            reduced, gathered.at[source], g_send.at[step - 1], g_recv.at[step - 1], peer(step)[1]
        ).wait_recv()
    for p in range(count):
        pooled[p * each : (p + 1) * each] = gathered[p].astype(f32)


    for side in range(2):

        @pl.when(jnp.logical_not(first if side else last))
        def _():
            for hop in range(HOPS):
                (down if side else up)(hop).wait_send()

    for copy in sends + copies:
        copy.wait_send()


def shards(nx, ny, tokens, lengths, ln_gain, w_qkv, w_out):
    local, width = tokens.shape[1:]
    images = lengths.shape[1]
    count = nx * ny
    chips = nx // 2
    each = images // count
    size = width // HEADS
    long = local + 2 * MAXLEN
    blocks = local // QBLOCK
    team = HEADS // GROUPS
    f32, bf16 = jnp.float32, jnp.bfloat16
    hbm = pl.BlockSpec(memory_space=pltpu.HBM)
    vmem = pl.BlockSpec(memory_space=pltpu.VMEM)
    dma = pltpu.SemaphoreType.DMA
    hidden, pooled = pl.pallas_call(
        functools.partial(block_kernel, nx, ny),
        out_shape=(
            jax.ShapeDtypeStruct((local, width), bf16), jax.ShapeDtypeStruct((images, width), f32),
        ),
        in_specs=[hbm] * 5,
        out_specs=(vmem, vmem),
        scratch_shapes=[
            pltpu.VMEM((1, images), jnp.int32), pltpu.VMEM((width // LANES, LANES), f32),
            pltpu.VMEM((long, width), bf16), pltpu.VMEM((long, width), bf16),
            pltpu.VMEM((width, 3 * width), bf16), pltpu.VMEM((width, width), bf16),
            pltpu.VMEM((1, width), f32),
            pltpu.VMEM((long, width), bf16),
            pltpu.VMEM((HEADS, 2 * LANES, local), bf16),
            pltpu.VMEM((HEADS, size + ONES, long), bf16),
            pltpu.VMEM((blocks, QBLOCK + 2 * MAXLEN, QBLOCK), f32),
            pltpu.VMEM((blocks * HEADS, 1, QBLOCK), f32),
            pltpu.VMEM((blocks * HEADS, size + ONES, QBLOCK), f32),
            pltpu.VMEM((team, local, QBLOCK), f32), pltpu.VMEM((team, local, QBLOCK), bf16),
            pltpu.VMEM((width, HOP), bf16),
            pltpu.VMEM((local, width), bf16),
            pltpu.VMEM((images, local), bf16), pltpu.VMEM((images, width), f32),
            pltpu.VMEM((count, each, width), bf16), pltpu.VMEM((count - 1, each, width), bf16),
            pltpu.VMEM((each, width), bf16), pltpu.VMEM((count, each, width), bf16),
            dma((CHUNKS,)), dma((CHUNKS,)),
            dma((max(chips - 1, 1), CHUNKS)), dma((max(chips - 1, 1), CHUNKS)),
            dma((chips, CHUNKS)), dma((chips, CHUNKS)),
            dma((2, HOPS)), dma((2, HOPS)),
            dma((count - 1,)), dma((count - 1,)), dma((count - 1,)), dma((count - 1,)),
            dma((3 + CHUNKS,)),
        ],
        compiler_params=pltpu.CompilerParams(
            collective_id=0, has_side_effects=True, vmem_limit_bytes=51 * 2**20 + count * 2**16
        ),
        name="block",
    )(tokens[0], lengths, ln_gain.reshape(width // LANES, LANES), w_qkv, w_out)
    return (hidden[None], pooled[None])


def solution(mesh):
    in_specs = (P("dp", ("sx", "sy"), None), P("dp", None), P(), P("dp", None), P("dp", None))
    out_specs = (P("dp", ("sx", "sy"), None), P("dp", None, None))
    body = functools.partial(shards, mesh.shape["sx"], mesh.shape["sy"])
    return jax.shard_map(body, mesh=mesh, in_specs=in_specs, out_specs=out_specs, check_vma=False)
```

```python
import functools

import jax
import jax.numpy as jnp
from jax import lax
from jax.experimental import pallas as pl
from jax.experimental.pallas import tpu as pltpu
from jax.sharding import PartitionSpec as P

HEADS = 16
MAXLEN = 512
MESH = pl.DeviceIdType.MESH
GROUPS = 2
WIDE_CHUNKS = 3 * GROUPS
CHUNKS = 4 * GROUPS
HOP = 128
HOPS = MAXLEN // HOP
NEAR = 2
QBLOCK = 256
LANES = 128
ONES = 16
FAR = -1e30


def remote(src, dst, send, recv, device):
    return pltpu.make_async_remote_copy(
        src_ref=src, dst_ref=dst, send_sem=send, recv_sem=recv, device_id=device, device_id_type=MESH
    )


def head_window(head, size):
    low = head * size // LANES * LANES
    high = -(-(head + 1) * size // LANES) * LANES
    return low, high - low


def block_kernel(
    nx, ny, tok, lengths_in, gain_in, wq, wo, hidden, pooled,
    lengths, gain, toks, normed, wq_full, wo_full, gains, keys, wide, turned, bias, top, acc, scores, probs, flat, context, onehot, sums, parts,
    landed, reduced, gathered,
    y_send, y_recv, x_send, x_recv, d_send, d_recv, h_send, h_recv, s_send, s_recv, g_send, g_recv, local_sem,
):
    sx, sy, dp = lax.axis_index("sx"), lax.axis_index("sy"), lax.axis_index("dp")
    chips = nx // 2
    chip, core = sx // 2, lax.rem(sx, 2)
    count = nx * ny
    shard = sx * ny + sy
    first, last = shard == 0, shard == count - 1
    f32, bf16 = jnp.float32, jnp.bfloat16

    local, width = tok.shape
    long = toks.shape[0]
    size = width // HEADS
    half = wq.shape[0]
    quarter = half // nx
    cols = width // GROUPS
    team = HEADS // GROUPS
    images = pooled.shape[0]
    each = images // count
    blocks = local // QBLOCK
    factor = size ** (-0.5) * 1.4426950408889634

    def peer(step):
        other = lax.rem(shard + step, count)
        return other, (other // ny, lax.rem(other, ny), dp)

    prev_id, next_id = peer(count - 1)[1], peer(1)[1]
    y_id = (sx, sy, 1 - dp)
    partner = (chip * 2 + 1 - core, sy, dp)

    def chip_id(step):
        return (lax.rem(chip + step, chips) * 2 + core, sy, dp)

    barrier = pltpu.get_barrier_semaphore()
    for device in [y_id] + [peer(step)[1] for step in range(1, count)]:
        pl.semaphore_signal(barrier, inc=1, device_id=device, device_id_type=MESH)
    own_tokens = pltpu.make_async_copy(tok, toks.at[pl.ds(MAXLEN, local)], local_sem.at[0])
    mine = pl.ds(pl.multiple_of(dp * half, half), half)

    def chunk(j):
        if j < WIDE_CHUNKS:
            return wq, pl.ds((j + 1) % 3 * width + j // 3 * cols, cols), wq_full, pl.ds(j * cols, cols)
        at = pl.ds((j - WIDE_CHUNKS) * cols, cols)
        return wo, at, wo_full, at

    own_weights = []
    for j in range(CHUNKS):
        part, at, full, to = chunk(j)
        own_weights.append(pltpu.make_async_copy(part.at[:, at], full.at[mine, to], local_sem.at[1 + j]))
    small = (
        pltpu.make_async_copy(lengths_in, lengths, local_sem.at[1 + CHUNKS]),
        pltpu.make_async_copy(gain_in, gain, local_sem.at[2 + CHUNKS]),
    )
    for copy in small:
        copy.start()
    own_tokens.start()
    for copy in own_weights:
        copy.start()
    pl.semaphore_wait(barrier, count)

    def rows(owner, slot):
        return pl.ds(pl.multiple_of(owner * half + slot * quarter, quarter), quarter)

    sends = []
    for j in range(CHUNKS):
        part, at, full, to = chunk(j)
        copy = remote(
            part.at[pl.ds(pl.multiple_of(sx * quarter, quarter), quarter), at],
            full.at[rows(dp, sx), to], y_send.at[j], y_recv.at[j], y_id,
        )
        copy.start()
        sends.append(copy)

    def place(side, hop):
        return MAXLEN + local + hop * HOP if side else MAXLEN - (hop + 1) * HOP

    def up(hop):
        return remote(
            tok.at[pl.ds(local - (hop + 1) * HOP, HOP)], toks.at[pl.ds(place(0, hop), HOP)],
            h_send.at[0, hop], h_recv.at[0, hop], next_id,
        )

    def down(hop):
        return remote(
            tok.at[pl.ds(hop * HOP, HOP)], toks.at[pl.ds(place(1, hop), HOP)],
            h_send.at[1, hop], h_recv.at[1, hop], prev_id,
        )

    for hop in range(HOPS):
        for side in range(2):

            @pl.when(jnp.logical_not(first if side else last))
            def _():
                (down if side else up)(hop).start()

    @pl.when(first)
    def _():
        toks[pl.ds(0, MAXLEN)] = jnp.zeros((MAXLEN, width), toks.dtype)

    @pl.when(last)
    def _():
        toks[pl.ds(MAXLEN + local, MAXLEN)] = jnp.zeros((MAXLEN, width), toks.dtype)

    for copy in small:
        copy.wait()
    for i in range(width // LANES):
        gains[:, pl.ds(i * LANES, LANES)] = gain[pl.ds(i, 1), :]

    def norm(start, amount, to):
        step = HOP

        @pl.loop(0, amount // step)
        def _(i):
            where = pl.ds(pl.multiple_of(start + i * step, step), step)
            values = toks[where].astype(f32)
            center = values - jnp.mean(values, axis=-1, keepdims=True)
            spread = jnp.mean(center * center, axis=-1, keepdims=True)
            normed[pl.ds(pl.multiple_of(to + i * step, step), step)] = (center * lax.rsqrt(spread + 1e-05) * gains[...]).astype(bf16)

    def project(start, amount, group, which, parts_of):
        at = pl.ds(pl.multiple_of((group * 3 + which) * cols, LANES), parts_of * cols)
        return jnp.dot(normed[pl.ds(start, amount)], wq_full[:, at], preferred_element_type=f32)

    def project_q(start, amount, group):
        columns = (project(start, amount, group, 2, 1) * factor).astype(bf16).T
        at = pl.ds(pl.multiple_of(start - MAXLEN, amount), amount)
        for head in range(team):
            low = head * size - head_window(head, size)[0]
            wide[group * team + head, pl.ds(low, size), at] = columns[head * size : (head + 1) * size]

    def project_kv(start, amount, group, places=None):
        both = project(start, amount, group, 0, 2).astype(bf16)
        columns = both[:, cols:].T
        places = places or (start,)
        each_part = amount // len(places)
        for i, to in enumerate(places):
            part = slice(i * each_part, (i + 1) * each_part)
            here = pl.ds(to, each_part)
            keys[here, pl.ds(pl.multiple_of(group * cols, LANES), cols)] = both[part, :cols]
            for head in range(team):
                turned[group * team + head, pl.ds(0, size), here] = columns[head * size : (head + 1) * size, part]

    def attend(block, group, segments, fresh, lane=0, lanes=QBLOCK):
        queries = pl.ds(pl.multiple_of(block * QBLOCK + lane, LANES), lanes)
        within = pl.ds(lane, lanes)
        total = sum(amount for _, amount in segments)
        offsets_at = [sum(amount for _, amount in segments[:i]) for i in range(len(segments))]
        some = (pl.ds(0, total), pl.ds(0, lanes))
        tops, shrinks = [], []
        for head in range(team):
            low, span = head_window(head, size)
            slot = group * team + head
            most = None
            for at, (start, amount) in zip(offsets_at, segments):
                shade = pl.ds(pl.multiple_of(start - block * QBLOCK, LANES), amount)
                found = jnp.dot(
                    keys[pl.ds(start, amount), pl.ds(pl.multiple_of(group * cols + low, LANES), span)],
                    wide[slot, pl.ds(0, span), queries], preferred_element_type=f32,
                ) + bias[block, shade, within]
                scores[head, pl.ds(at, amount), pl.ds(0, lanes)] = found
                peak = jnp.max(found, axis=0, keepdims=True)
                most = peak if most is None else jnp.maximum(most, peak)
            tops.append(most)
        for head in range(team):
            where = block * HEADS + group * team + head
            new = tops[head]
            if not fresh:
                old = top[where, :, within]
                new = jnp.maximum(old, new)
                shrinks.append(jnp.exp2(old - new))
            top[where, :, within] = new
            probs[(head,) + some] = jnp.exp2(scores[(head,) + some] - new).astype(bf16)
        for head in range(team):
            slot = group * team + head
            where = block * HEADS + slot
            mixed = None
            for at, (start, amount) in zip(offsets_at, segments):
                part = jnp.dot(
                    turned[slot, :, pl.ds(start, amount)], probs[head, pl.ds(at, amount), pl.ds(0, lanes)],
                    preferred_element_type=f32,
                )
                mixed = part if mixed is None else mixed + part
            if not fresh:
                mixed = acc[where, :, within] * shrinks[head] + mixed
            acc[where, :, within] = mixed

    own_tokens.wait()
    norm(MAXLEN, local, MAXLEN)

    wide[...] = jnp.zeros(wide.shape, bf16)
    turned[:, pl.ds(size, ONES), :] = jnp.ones((HEADS, ONES, long), bf16)
    row_lengths = lengths[...].astype(f32)
    to = lax.broadcasted_iota(jnp.int32, (images, images), 0)
    of = lax.broadcasted_iota(jnp.int32, (images, images), 1)
    offsets = jnp.sum(jnp.where(of < to, row_lengths, 0.0), axis=1, keepdims=True)
    amounts = jnp.sum(jnp.where(of == to, row_lengths, 0.0), axis=1, keepdims=True)
    ends = offsets + amounts
    base = shard * local
    spots = (base + lax.broadcasted_iota(jnp.int32, (1, local), 1)).astype(f32)
    inside = (offsets <= spots) & (spots < ends)
    onehot[...] = jnp.where(inside, 1.0, 0.0).astype(bf16)
    begin = jnp.max(jnp.where(inside, offsets, 0.0), axis=0, keepdims=True)
    end = jnp.max(jnp.where(inside, ends, 0.0), axis=0, keepdims=True)
    for block in range(blocks):
        mine_begin = begin[:, block * QBLOCK : (block + 1) * QBLOCK]
        mine_end = end[:, block * QBLOCK : (block + 1) * QBLOCK]
        step = 64

        @pl.loop(0, bias.shape[1] // step)
        def _(i):
            at = pl.multiple_of(i * step, step)
            spot = base - MAXLEN + block * QBLOCK + at + lax.broadcasted_iota(jnp.int32, (step, QBLOCK), 0)
            spot = spot.astype(f32)
            allowed = (spot >= mine_begin) & (spot < mine_end)
            bias[block, pl.ds(at, step)] = jnp.where(allowed, 0.0, FAR)

    def relay_y(j):
        here = chunk(j)[2].at[rows(1 - dp, sx), chunk(j)[3]]
        remote(here, here, y_send.at[j], y_recv.at[j], y_id).wait_recv()
        for step in range(1, chips):
            copy = remote(here, here, x_send.at[step - 1, j], x_recv.at[step - 1, j], chip_id(step))
            copy.start()
            sends.append(copy)
        copy = remote(here, here, d_send.at[0, j], d_recv.at[0, j], partner)
        copy.start()
        sends.append(copy)

    def relay_x(j):
        for step in range(1, chips):
            slot = lax.rem(chip + chips - step, chips) * 2 + core
            here = chunk(j)[2].at[rows(1 - dp, slot), chunk(j)[3]]
            remote(here, here, x_send.at[step - 1, j], x_recv.at[step - 1, j], y_id).wait_recv()
            copy = remote(here, here, d_send.at[step, j], d_recv.at[step, j], partner)
            copy.start()
            sends.append(copy)

    def complete(j):
        for step in range(chips):
            slot = lax.rem(chip + chips - step, chips) * 2 + 1 - core
            here = chunk(j)[2].at[rows(1 - dp, slot), chunk(j)[3]]
            remote(here, here, d_send.at[step, j], d_recv.at[step, j], partner).wait_recv()

    def arrived(hop):
        for side in range(2):

            @pl.when(jnp.logical_not(last if side else first))
            def _():
                (down if side else up)(hop).wait_recv()

            norm(place(side, hop), HOP, place(side, hop) if hop < NEAR else side * HOP)

    near = NEAR * HOP

    near_starts = (MAXLEN - near, MAXLEN + local)

    def near_kv(group):
        for side in range(2):
            project_kv(near_starts[side], near, group)

    def near_attend(group):
        @pl.loop(0, blocks)
        def _(block):
            attend(block, group, [(start, near) for start in near_starts], False)

    def own_attend(group):
        @pl.loop(0, blocks)
        def _(block):
            attend(block, group, [(MAXLEN, local)], True)

    def ready(*chunks):
        for j in chunks:
            complete(j)
            own_weights[j].wait()

    def far(hop):
        arrived(hop)

        @pl.loop(0, GROUPS)
        def _(group):
            project_kv(0, 2 * HOP, group, (place(0, hop), place(1, hop)))
            for side in range(2):
                lanes = min(QBLOCK, (HOPS - hop) * HOP)
                spot = [(place(side, hop), HOP)]
                attend(side * (blocks - 1), group, spot, False, side * (QBLOCK - lanes), lanes)

    tile = cols

    def finish(start, amount):
        for at in range(start, start + amount, HOP):
            block, lane = at // QBLOCK, at % QBLOCK

            @pl.loop(0, GROUPS)
            def _(group):
                for head in range(team):
                    where = block * HEADS + group * team + head
                    share = 1.0 / acc[where, pl.ds(size, 1), pl.ds(lane, HOP)]
                    rows_at = pl.ds(pl.multiple_of(group * cols + head * size, size), size)
                    flat[rows_at] = (acc[where, pl.ds(0, size), pl.ds(lane, HOP)] * share).astype(bf16)

            context[pl.ds(at, HOP)] = flat[...].T

    def emit(starts, amount):
        @pl.loop(0, width // tile)
        def _(c):
            at = pl.ds(pl.multiple_of(c * tile, LANES), tile)
            lhs = jnp.concatenate([context[pl.ds(start, amount)] for start in starts], axis=0)
            mixed = jnp.dot(lhs, wo_full[:, at], preferred_element_type=f32)
            for i, start in enumerate(starts):
                residual = toks[pl.ds(MAXLEN + start, amount), at].astype(f32)
                hidden[pl.ds(start, amount), at] = (residual + mixed[i * amount : (i + 1) * amount]).astype(bf16)

    def relay(j):
        relay_y(j)
        if j:
            relay_x(j - 1)

    for j in range(4):
        relay(j)
    ready(0, 1)
    project_kv(MAXLEN, local, 0)
    ready(2)
    project_q(MAXLEN, local, 0)
    relay(4)
    own_attend(0)
    relay(5)
    arrived(0)
    relay_x(5)
    arrived(1)
    near_kv(0)
    ready(3, 4)
    project_kv(MAXLEN, local, 1)
    relay_y(6)
    near_attend(0)
    ready(5)
    project_q(MAXLEN, local, 1)
    relay_x(6)
    relay_y(7)
    own_attend(1)
    near_kv(1)
    relay_x(7)
    near_attend(1)
    for hop in range(NEAR, HOPS - 1):
        far(hop)
    ready(*range(WIDE_CHUNKS, CHUNKS))
    finish(HOP, local - 2 * HOP)
    emit((HOP,), local - 2 * HOP)
    inner = slice(HOP, local - HOP)
    sums[...] = jnp.dot(onehot[:, inner], hidden[inner], preferred_element_type=f32)
    far(HOPS - 1)
    for start in (0, local - HOP):
        finish(start, HOP)
    emit((0, local - HOP), HOP)

    found = sums[...]
    for edge in (slice(0, HOP), slice(local - HOP, local)):
        found = found + jnp.dot(onehot[:, edge], hidden[edge], preferred_element_type=f32)
    sums[...] = found * (1.0 / amounts)
    for p in range(count):
        parts[p] = sums[p * each : (p + 1) * each].astype(bf16)

    copies = []
    for step in range(1, count):
        other, ident = peer(step)
        copy = remote(parts.at[other], landed.at[step - 1], s_send.at[step - 1], s_recv.at[step - 1], ident)
        copy.start()
        copies.append(copy)
    value = parts[shard].astype(f32)
    for step in range(1, count):
        copies[step - 1].wait_recv()
        value = value + landed[step - 1].astype(f32)
    reduced[...] = value.astype(bf16)
    gathered[shard] = value.astype(bf16)
    for step in range(1, count):
        copy = remote(reduced, gathered.at[shard], g_send.at[step - 1], g_recv.at[step - 1], peer(step)[1])
        copy.start()
        copies.append(copy)
    for step in range(1, count):
        source = peer(count - step)[0]
        remote(
            reduced, gathered.at[source], g_send.at[step - 1], g_recv.at[step - 1], peer(step)[1]
        ).wait_recv()
    for p in range(count):
        pooled[p * each : (p + 1) * each] = gathered[p].astype(f32)


    for side in range(2):

        @pl.when(jnp.logical_not(first if side else last))
        def _():
            for hop in range(HOPS):
                (down if side else up)(hop).wait_send()

    for copy in sends + copies:
        copy.wait_send()


def shards(nx, ny, tokens, lengths, ln_gain, w_qkv, w_out):
    local, width = tokens.shape[1:]
    images = lengths.shape[1]
    count = nx * ny
    chips = nx // 2
    each = images // count
    size = width // HEADS
    long = local + 2 * MAXLEN
    blocks = local // QBLOCK
    team = HEADS // GROUPS
    f32, bf16 = jnp.float32, jnp.bfloat16
    hbm = pl.BlockSpec(memory_space=pltpu.HBM)
    vmem = pl.BlockSpec(memory_space=pltpu.VMEM)
    dma = pltpu.SemaphoreType.DMA
    hidden, pooled = pl.pallas_call(
        functools.partial(block_kernel, nx, ny),
        out_shape=(
            jax.ShapeDtypeStruct((local, width), bf16), jax.ShapeDtypeStruct((images, width), f32),
        ),
        in_specs=[hbm] * 5,
        out_specs=(vmem, vmem),
        scratch_shapes=[
            pltpu.VMEM((1, images), jnp.int32), pltpu.VMEM((width // LANES, LANES), f32),
            pltpu.VMEM((long, width), bf16), pltpu.VMEM((long, width), bf16),
            pltpu.VMEM((width, 3 * width), bf16), pltpu.VMEM((width, width), bf16),
            pltpu.VMEM((1, width), f32),
            pltpu.VMEM((long, width), bf16),
            pltpu.VMEM((HEADS, 2 * LANES, local), bf16),
            pltpu.VMEM((HEADS, size + ONES, long), bf16),
            pltpu.VMEM((blocks, QBLOCK + 2 * MAXLEN, QBLOCK), f32),
            pltpu.VMEM((blocks * HEADS, 1, QBLOCK), f32),
            pltpu.VMEM((blocks * HEADS, size + ONES, QBLOCK), f32),
            pltpu.VMEM((team, local, QBLOCK), f32), pltpu.VMEM((team, local, QBLOCK), bf16),
            pltpu.VMEM((width, HOP), bf16),
            pltpu.VMEM((local, width), bf16),
            pltpu.VMEM((images, local), bf16), pltpu.VMEM((images, width), f32),
            pltpu.VMEM((count, each, width), bf16), pltpu.VMEM((count - 1, each, width), bf16),
            pltpu.VMEM((each, width), bf16), pltpu.VMEM((count, each, width), bf16),
            dma((CHUNKS,)), dma((CHUNKS,)),
            dma((max(chips - 1, 1), CHUNKS)), dma((max(chips - 1, 1), CHUNKS)),
            dma((chips, CHUNKS)), dma((chips, CHUNKS)),
            dma((2, HOPS)), dma((2, HOPS)),
            dma((count - 1,)), dma((count - 1,)), dma((count - 1,)), dma((count - 1,)),
            dma((3 + CHUNKS,)),
        ],
        compiler_params=pltpu.CompilerParams(
            collective_id=0, has_side_effects=True, vmem_limit_bytes=51 * 2**20 + count * 2**16
        ),
        name="block",
    )(tokens[0], lengths, ln_gain.reshape(width // LANES, LANES), w_qkv, w_out)
    return (hidden[None], pooled[None])


def solution(mesh):
    in_specs = (P("dp", ("sx", "sy"), None), P("dp", None), P(), P("dp", None), P("dp", None))
    out_specs = (P("dp", ("sx", "sy"), None), P("dp", None, None))
    body = functools.partial(shards, mesh.shape["sx"], mesh.shape["sy"])
    return jax.shard_map(body, mesh=mesh, in_specs=in_specs, out_specs=out_specs, check_vma=False)
```
